32 devices in a mesh: node: 8 (over z, y), local: 4 (over x, core).
Axes of the slice: x: 2, y: 2, z: 4, core: 2. Of those that a mesh axis runs over, the one named last changes fastest.
Arguments:
- tokens: bfloat16 [4096, 4096], P(('node', 'local')), may hold values from -6 to 6
- expert_ids: int32 [4096, 8], P(('node', 'local')), may hold values from 0 to 31, all different within a row; in each aligned block of 128 rows (0 to 127, 128 to 255, ...) at most 40 rows name the same one
- gate_scores: float32 [4096, 8], P(('node', 'local')), may hold values from 0.03 to 0.4
- w_gate: bfloat16 [32, 4096, 768], P(('node', 'local')), may hold values from -0.09375 to 0.09375
- w_up: bfloat16 [32, 4096, 768], P(('node', 'local')), may hold values from -0.09375 to 0.09375
- w_down: bfloat16 [32, 768, 4096], P(('node', 'local')), may hold values from -0.21875 to 0.21875
Outputs:
- mixed: bfloat16 [4096, 4096], P(('node', 'local'))
The draws below stay inside these ranges and needn't reach their ends.
Inputs may be any that keep to these rules, and one draw needn't show every extreme that they name: `expert_ids`: each row names 8 different experts. Among the 128 rows of one device no expert is named more than 40 times, and that many is reached on some device.
All inputs are finite; a program needn't handle non-finite values.
Results may differ from the reference program's by a relative error of at most 0.0058.
Values may be sent and summed in bfloat16 or wider, within the bound.
No kernel may reach another device: no remote copies, remote signals or barrier semaphores. Data moves between devices by JAX's collectives and lax.ppermute only.
A program may use at most 128 MiB of HBM per device.

```python
import math
import jax
import jax.numpy as jnp
import numpy as np
from jax import lax

D = 4096
FF = 768
TOP = 8
TOK_DEV = 128
EXPERTS = 32
CAP = 40
TOKENS = 4096


def level_of(stream_key, extent, shards, least, largest):
    def one(position, parts):
        steps = jax.random.uniform(jax.random.fold_in(jax.random.fold_in(stream_key, 6), position), (parts,), jnp.float32, least / len(shards), largest / len(shards))
        return jnp.repeat(jnp.exp(steps), extent[position] // parts).reshape((-1,) + (1,) * (len(extent) - position - 1))

    factor_of = one(*shards[0])
    for cut in shards[1:]:
        factor_of = factor_of * one(*cut)
    return factor_of


def routed_block(rng, own, number, rows, number_of, top, limit, lean):
    ranking = jax.random.permutation(rng, number_of)
    packed, ordinary = shares(number_of, rows * top, limit, lean, True), shares(number_of, rows * top, limit, lean, False)
    places = jnp.arange(number_of)

    def named(sizes, turn):
        used = int((sizes > 0).sum())
        fixed = max(1, used // 4)
        moved = fixed + (places - fixed + turn * (used - fixed)) % max(1, number_of - fixed)
        return jnp.zeros((number_of,), jnp.int32).at[ranking[jnp.where(places < fixed, places, moved)]].set(jnp.asarray(sizes, jnp.int32))

    sizes = jnp.where(number % 4 == 0, named(packed, number // 4), named(ordinary, number - number // 4 - 1))
    mixed = jax.random.permutation(jax.random.fold_in(own, 3), number_of)
    donor, receiver = mixed[0:number_of // 2 * 2:2], mixed[1:number_of // 2 * 2:2]
    slack = jnp.minimum(sizes[donor] - 1, limit - sizes[receiver]) // 2
    slack = jnp.where((donor == ranking[0]) | (receiver == ranking[0]) | (sizes[receiver] == 0), 0, jnp.maximum(slack, 0))
    moved = jax.random.randint(jax.random.fold_in(own, 4), (number_of // 2,), 0, 1 << 20) % (slack + 1)
    sizes = sizes.at[donor].add(-moved).at[receiver].add(moved)
    items = jnp.searchsorted(jnp.cumsum(sizes), jnp.arange(rows * top), side="right").astype(jnp.int32)
    grid = items.reshape(top, rows).T
    grid = grid[jax.random.permutation(jax.random.fold_in(own, 1), rows)]
    turn = jax.random.randint(jax.random.fold_in(own, 2), (rows, 1), 0, top)
    return jnp.take_along_axis(grid, (jnp.arange(top)[None, :] + turn) % top, axis=1)


def shares(amount, total, limit, skew, full):
    loads = [(1 << 20) // math.isqrt(grade ** skew) + 1 for grade in range(1, amount + 1)]
    largest = limit if full else min(limit, max(-(-total // amount), total * loads[0] // sum(loads)))
    least = 1 if total - largest >= amount - 1 else 0
    holding, surplus = [largest] + [least] * (amount - 1), total - largest - least * (amount - 1)
    while surplus > 0:
        candidates = [i for i in range(1, amount) if holding[i] < largest] or [i for i in range(1, amount) if holding[i] < limit]
        whole, budget = sum([loads[i] for i in candidates]), surplus
        for i in candidates:
            extra = min(limit - holding[i], max(1, budget * loads[i] // whole), surplus)
            holding[i] = holding[i] + extra
            surplus = surplus - extra
    return np.array(holding)


def normal_values(rng, extent, scale, reach, cuts=(), held_as=jnp.bfloat16):
    entries = jax.random.normal(rng, extent, jnp.float32) * scale
    if len(cuts) > 0:
        entries = level_of(rng, extent, cuts, -0.22, 0.18) * entries
    return jnp.clip(entries, min=-reach, max=reach).astype(held_as)


def setup_inputs(seed: int = 0) -> dict:
    key_list = jax.random.split(jax.random.key(seed), 7)
    tokens = normal_values(key_list[0], (TOKENS, D), 1.0, 6.0, ((0, 32),))
    expert_ids_keys = jax.random.split(jax.random.fold_in(key_list[1], 1), TOKENS // TOK_DEV)
    expert_ids_turns = jax.random.permutation(jax.random.fold_in(key_list[1], 3), TOKENS // TOK_DEV)
    expert_ids = jax.vmap(lambda own, number: routed_block(jax.random.fold_in(key_list[1], 2), own, number, TOK_DEV, EXPERTS, TOP, CAP, 1))(expert_ids_keys, expert_ids_turns).reshape((TOKENS, TOP))
    gate_scores = jnp.clip(jnp.exp(math.log(0.4) - 2.5902672 * jax.random.uniform(key_list[2], (TOKENS, TOP), jnp.float32) ** level_of(key_list[2], (TOKENS, TOP), ((0, 32),), -0.2, 0.2)), 0.03, 0.4)
    w_gate = normal_values(key_list[3], (EXPERTS, D, FF), D ** -0.5, 0.09375, ((0, 32),))
    w_up = normal_values(key_list[4], (EXPERTS, D, FF), D ** -0.5, 0.09375, ((0, 32),))
    w_down = normal_values(key_list[5], (EXPERTS, FF, D), FF ** -0.5, 0.21875, ((0, 32),))
    return dict(tokens=tokens, expert_ids=expert_ids, gate_scores=gate_scores, w_gate=w_gate, w_up=w_up, w_down=w_down)


def reference(tokens, expert_ids, gate_scores, w_gate, w_up, w_down):
    flat_ids = expert_ids.reshape(-1)
    flat_gates = gate_scores.reshape(-1)
    slot_limit = EXPERTS * CAP

    def add_expert(totals, expert):
        chosen = flat_ids == expert
        positions = jnp.nonzero(chosen, size=slot_limit, fill_value=0)[0].astype(jnp.int32)
        live_rows = jnp.arange(slot_limit, dtype=jnp.int32) < jnp.sum(chosen.astype(jnp.int32))
        token_rows = positions // TOP
        inputs = tokens[token_rows]
        gate_part = jnp.dot(inputs, w_gate[expert], preferred_element_type=jnp.float32)
        up_part = jnp.dot(inputs, w_up[expert], preferred_element_type=jnp.float32)
        hidden = (jax.nn.silu(gate_part) * up_part).astype(jnp.bfloat16)
        output = jnp.dot(hidden, w_down[expert], preferred_element_type=jnp.float32).astype(jnp.bfloat16).astype(jnp.float32)
        weights = jnp.where(live_rows, flat_gates[positions], jnp.zeros((), jnp.float32))
        totals = totals.at[token_rows].add(weights[:, None] * output)
        return totals, None

    start = jnp.zeros((TOKENS, D), jnp.float32)
    totals, unused = lax.scan(add_expert, start, jnp.arange(EXPERTS, dtype=jnp.int32))
    return totals.astype(jnp.bfloat16)
```

```python
import functools

import jax
import jax.numpy as jnp
import numpy as np
from jax import lax
from jax.experimental import pallas as pl
from jax.experimental.pallas import tpu as pltpu
from jax.sharding import PartitionSpec as P


AXES = ("node", "local")
BF16 = jnp.bfloat16
F32 = jnp.float32
COLUMN_STEPS = 4


def planes_of(mesh):
    flat = mesh.devices.reshape(-1)
    depth = np.array([getattr(d, "coords", (0, 0, 0))[2] for d in flat])
    count = len(set(depth.tolist()))
    rows = depth.reshape(count, -1) if flat.size % count == 0 else depth.reshape(1, -1)
    if count > 1 and all(len(set(r.tolist())) == 1 for r in rows):
        return count
    return 1


def picks(table, capacity):
    experts, count = table.shape
    slots = lax.broadcasted_iota(jnp.int32, (capacity, count), 0).astype(F32)
    return [table[e : e + 1, :] == slots for e in range(experts)]


def pack_kernel(capacity, facts_ref, rows_ref, *outs):
    experts = len(outs)
    chosen = jnp.concatenate(
        [jnp.where(r, 1.0, 0.0) for r in picks(facts_ref[:experts, :], capacity)], axis=0
    ).astype(BF16)
    packed = jnp.dot(chosen, rows_ref[...], preferred_element_type=F32).astype(BF16)
    for e, out in enumerate(outs):
        out[...] = packed[e * capacity : (e + 1) * capacity, :]


def pack(facts, rows, capacity):
    experts, (count, features) = facts.shape[0] // 2, rows.shape
    step = features // COLUMN_STEPS
    return pl.pallas_call(
        functools.partial(pack_kernel, capacity),
        grid=(COLUMN_STEPS,),
        in_specs=[
            pl.BlockSpec(facts.shape, lambda i: (0, 0)),
            pl.BlockSpec((count, step), lambda i: (0, i)),
        ],
        out_specs=[pl.BlockSpec((capacity, step), lambda i: (0, i))] * experts,
        out_shape=[jax.ShapeDtypeStruct((capacity, features), BF16)] * experts,
        cost_estimate=pl.CostEstimate(
            flops=2 * experts * capacity * count * features,
            bytes_accessed=2 * (experts * capacity + count) * features,
            transcendentals=0,
        ),
    )(facts, rows)


def mix_kernel(capacity, experts, facts_ref, *refs):
    *rows, out_ref = refs
    weight = jnp.concatenate(
        [
            jnp.where(r, facts_ref[experts + e : experts + e + 1, :], 0.0)
            for e, r in enumerate(picks(facts_ref[:experts, :], capacity))
        ],
        axis=0,
    )
    high = weight.astype(BF16)
    low = (weight - high.astype(F32)).astype(BF16)
    dims = (((0,), (0,)), ((), ()))
    value = jnp.concatenate([r[...] for r in rows[:experts]], axis=0)
    total = lax.dot_general(high, value, dims, preferred_element_type=F32)
    total += lax.dot_general(low, value, dims, preferred_element_type=F32)
    for other in rows[experts:]:
        total += other[...].astype(F32)
    out_ref[...] = total.astype(out_ref.dtype)


def mix(facts, rows, others, capacity):
    experts, count, features = facts.shape[0] // 2, facts.shape[1], rows[0].shape[1]
    step = features // COLUMN_STEPS
    tall = [pl.BlockSpec((r.shape[0], step), lambda i: (0, i)) for r in [*rows, *others]]
    return pl.pallas_call(
        functools.partial(mix_kernel, capacity, experts),
        grid=(COLUMN_STEPS,),
        in_specs=[pl.BlockSpec(facts.shape, lambda i: (0, 0)), *tall],
        out_specs=pl.BlockSpec((count, step), lambda i: (0, i)),
        out_shape=jax.ShapeDtypeStruct((count, features), BF16),
        cost_estimate=pl.CostEstimate(
            flops=4 * experts * capacity * count * features,
            bytes_accessed=2 * (experts * capacity + 2 * count) * features,
            transcendentals=0,
        ),
    )(facts, *rows, *others)


def ffn_kernel(pieces, capacity, gate_ref, up_ref, down_ref, *refs):
    rows, outs, (held, total) = refs[:pieces], refs[pieces : 2 * pieces], refs[2 * pieces :]
    step, last = pl.program_id(0), pl.num_programs(0) - 1

    @pl.when(step == 0)
    def _():
        for m in range(pieces):
            held[m * capacity : (m + 1) * capacity, :] = rows[m][...]

    value = held[...]
    gate_part = jnp.dot(value, gate_ref[0], preferred_element_type=F32)
    up_part = jnp.dot(value, up_ref[0], preferred_element_type=F32)
    hidden = (gate_part / (1.0 + jnp.exp(-gate_part)) * up_part).astype(BF16)
    part = jnp.dot(hidden, down_ref[0], preferred_element_type=F32)

    @pl.when(step == 0)
    def _():
        total[...] = part

    @pl.when((step > 0) & (step < last))
    def _():
        total[...] += part

    @pl.when((step > 0) & (step == last))
    def _():
        total[...] += part

    @pl.when(step == last)
    def _():
        for m in range(pieces):
            outs[m][...] = total[m * capacity : (m + 1) * capacity, :].astype(BF16)


def ffn(rows, w_gate, w_up, w_down):
    pieces, (capacity, features) = len(rows), rows[0].shape
    hidden = w_gate.shape[2]
    tile = 256 if hidden % 256 == 0 else hidden
    steps = hidden // tile
    whole = pl.BlockSpec((capacity, features), lambda i: (0, 0))
    count = pieces * capacity
    return pl.pallas_call(
        functools.partial(ffn_kernel, pieces, capacity),
        grid=(steps,),
        in_specs=[
            pl.BlockSpec((1, features, tile), lambda i: (0, 0, i)),
            pl.BlockSpec((1, features, tile), lambda i: (0, 0, i)),
            pl.BlockSpec((1, tile, features), lambda i: (0, i, 0)),
        ]
        + [whole] * pieces,
        out_specs=[whole] * pieces,
        out_shape=[jax.ShapeDtypeStruct((capacity, features), BF16)] * pieces,
        scratch_shapes=[
            pltpu.VMEM((count, features), BF16),
            pltpu.VMEM((count, features), F32),
        ],
        compiler_params=pltpu.CompilerParams(vmem_limit_bytes=56 * 1024 * 1024),
        cost_estimate=pl.CostEstimate(
            flops=6 * count * features * hidden,
            bytes_accessed=2 * features * (3 * hidden + 2 * count),
            transcendentals=count * hidden,
        ),
    )(w_gate, w_up, w_down, *rows)


def layer(planes, size, tokens, expert_ids, gate_scores, w_gate, w_up, w_down):
    width = size // planes
    token_count, _ = tokens.shape
    top_count = expert_ids.shape[1]
    capacity = 5 * token_count * top_count // (4 * size)
    me = lax.axis_index(AXES)
    plane, place = me // width, me % width
    xor = width & (width - 1) == 0

    def partner(spot, step):
        return spot ^ step if xor else (spot + step) % width

    def along(x, step):
        return lax.ppermute(x, AXES, [(i, (i + step * width) % size) for i in range(size)])

    def across(x, step, back):
        pairs = [(i, i // width * width + partner(i % width, step)) for i in range(size)]
        return lax.ppermute(x, AXES, [p[::-1] for p in pairs] if back else pairs)

    experts = jnp.arange(size, dtype=jnp.int32)
    experts = experts // width * width + partner(place, experts % width)
    match = expert_ids.T[None, :, :] == experts[:, None, None]
    named = jnp.any(match, axis=1)
    score = jnp.sum(jnp.where(match, gate_scores.T[None, :, :], 0.0), axis=1)
    earlier = jnp.triu(jnp.ones((token_count, token_count), BF16), 1)
    rank = jnp.dot(named.astype(BF16), earlier, preferred_element_type=F32)
    rank = jnp.where(named, rank, -1.0)
    table = jnp.stack([rank.reshape(planes, width, -1), score.reshape(planes, width, -1)], axis=1)
    table = table.reshape(planes, 2 * width, token_count)

    def facts_of(target):
        return lax.dynamic_index_in_dim(table, target, 0, keepdims=False)

    blocks, facts = [tokens], [facts_of(plane)]
    for s in range(1, planes):
        facts.append(along(facts_of((plane + s) % planes), s))
    for _ in range(1, planes):
        blocks.append(along(blocks[-1], 1))

    outputs = []
    for s in range(planes):
        rows = pack(facts[s], blocks[s], capacity)
        rows = [rows[0]] + [across(rows[m], m, False) for m in range(1, width)]
        outputs.append(ffn(rows, w_gate, w_up, w_down))
    others = []
    for s in [*range(1, planes), 0]:
        rows = outputs[s]
        rows = [rows[0]] + [across(rows[m], m, True) for m in range(1, width)]
        part = mix(facts[s], rows, others, capacity)
        if s:
            others = [along(part, 1)]
    return part


def solution(mesh):
    split = P(AXES, None)
    whole = P(AXES, None, None)
    planes, size = planes_of(mesh), mesh.devices.size

    def step(*arrays):
        return layer(planes, size, *arrays)

    return jax.shard_map(
        step,
        mesh=mesh,
        in_specs=(split, split, split, whole, whole, whole),
        out_specs=split,
        check_vma=False,
    )
```

```python
import functools

import jax
import jax.numpy as jnp
import numpy as np
from jax import lax
from jax.experimental import pallas as pl
from jax.experimental.pallas import tpu as pltpu
from jax.sharding import PartitionSpec as P


AXES = ("node", "local")
BF16 = jnp.bfloat16
F32 = jnp.float32
COLUMN_STEPS = 2
HALVES = 2


def planes_of(mesh):
    flat = mesh.devices.reshape(-1)
    depth = np.array([getattr(d, "coords", (0, 0, 0))[2] for d in flat])
    count = len(set(depth.tolist()))
    rows = depth.reshape(count, -1) if flat.size % count == 0 else depth.reshape(1, -1)
    if count > 1 and all(len(set(r.tolist())) == 1 for r in rows):
        return count
    return 1


def parts_of(s, planes):
    return HALVES if 0 < s == planes - 1 else 1


def picks(table, capacity):
    experts, count = table.shape
    slots = lax.broadcasted_iota(jnp.int32, (capacity, count), 0).astype(F32)
    return [table[e : e + 1, :] == slots for e in range(experts)]


def pack_kernel(capacity, facts_ref, rows_ref, *outs):
    experts = len(outs)
    chosen = jnp.concatenate(
        [jnp.where(r, 1.0, 0.0) for r in picks(facts_ref[:experts, :], capacity)], axis=0
    ).astype(BF16)
    packed = jnp.dot(chosen, rows_ref[...], preferred_element_type=F32).astype(BF16)
    for e, out in enumerate(outs):
        out[...] = packed[e * capacity : (e + 1) * capacity, :]


def pack(facts, rows, capacity):
    experts, (count, features) = facts.shape[0] // 2, rows.shape
    step = features // COLUMN_STEPS
    return pl.pallas_call(
        functools.partial(pack_kernel, capacity),
        grid=(COLUMN_STEPS,),
        in_specs=[
            pl.BlockSpec(facts.shape, lambda i: (0, 0)),
            pl.BlockSpec((count, step), lambda i: (0, i)),
        ],
        out_specs=[pl.BlockSpec((capacity, step), lambda i: (0, i))] * experts,
        out_shape=[jax.ShapeDtypeStruct((capacity, features), BF16)] * experts,
        cost_estimate=pl.CostEstimate(
            flops=2 * experts * capacity * count * features,
            bytes_accessed=2 * (experts * capacity + count) * features,
            transcendentals=0,
        ),
    )(facts, rows)


def mix_kernel(capacity, experts, extra, facts_ref, *refs):
    out_ref = refs[-1]
    rows = refs[:experts]
    weight = jnp.concatenate(
        [
            jnp.where(r, facts_ref[experts + e : experts + e + 1, :], 0.0)
            for e, r in enumerate(picks(facts_ref[:experts, :], capacity))
        ],
        axis=0,
    )
    high = weight.astype(BF16)
    low = (weight - high.astype(F32)).astype(BF16)
    dims = (((0,), (0,)), ((), ()))
    value = jnp.concatenate([r[...] for r in rows], axis=0)
    total = lax.dot_general(high, value, dims, preferred_element_type=F32)
    total += lax.dot_general(low, value, dims, preferred_element_type=F32)
    for half, other in enumerate(refs[experts:-1]):
        if extra == 1:
            total += other[...].astype(F32)
        else:
            total += jnp.where(pl.program_id(0) == half, other[...].astype(F32), 0.0)
    out_ref[...] = total.astype(out_ref.dtype)


def mix(facts, rows, others, capacity, step, first, steps):
    experts, count = facts.shape[0] // 2, facts.shape[1]
    specs = [pl.BlockSpec(facts.shape, lambda i: (0, 0))]
    specs += [pl.BlockSpec((r.shape[0], step), lambda i: (0, first + i)) for r in rows]
    specs += [pl.BlockSpec((count, step), lambda i: (0, 0)) for _ in others]
    return pl.pallas_call(
        functools.partial(mix_kernel, capacity, experts, len(others)),
        grid=(steps,),
        in_specs=specs,
        out_specs=pl.BlockSpec((count, step), lambda i: (0, i)),
        out_shape=jax.ShapeDtypeStruct((count, steps * step), BF16),
        cost_estimate=pl.CostEstimate(
            flops=4 * experts * capacity * count * step * steps,
            bytes_accessed=2 * (experts * capacity + 2 * count) * step * steps,
            transcendentals=0,
        ),
    )(facts, *rows, *others)


def ffn_kernel(pieces, capacity, gate_ref, up_ref, down_ref, *refs):
    rows, outs, (held, total) = refs[:pieces], refs[pieces:-2], refs[-2:]
    step, last = pl.program_id(0), pl.num_programs(0) - 1

    @pl.when(step == 0)
    def _():
        for m in range(pieces):
            held[m * capacity : (m + 1) * capacity, :] = rows[m][...]

    value = held[...]
    gate_part = jnp.dot(value, gate_ref[0], preferred_element_type=F32)
    up_part = jnp.dot(value, up_ref[0], preferred_element_type=F32)
    hidden = (gate_part / (1.0 + jnp.exp(-gate_part)) * up_part).astype(BF16)
    part = jnp.dot(hidden, down_ref[0], preferred_element_type=F32)

    @pl.when(step == 0)
    def _():
        total[...] = part

    @pl.when((step > 0) & (step < last))
    def _():
        total[...] += part

    @pl.when((step > 0) & (step == last))
    def _():
        total[...] += part

    @pl.when(step == last)
    def _():
        for k, out in enumerate(outs):
            part, m = divmod(k, pieces)
            columns = slice(part * out.shape[1], (part + 1) * out.shape[1])
            out[...] = total[m * capacity : (m + 1) * capacity, columns].astype(BF16)


def ffn(rows, w_gate, w_up, w_down, parts):
    pieces, (capacity, features) = len(rows), rows[0].shape
    hidden = w_gate.shape[2]
    tile = 256 if hidden % 256 == 0 else hidden
    steps = hidden // tile
    whole = pl.BlockSpec((capacity, features), lambda i: (0, 0))
    piece = (capacity, features // parts)
    count = pieces * capacity
    outs = pl.pallas_call(
        functools.partial(ffn_kernel, pieces, capacity),
        grid=(steps,),
        in_specs=[
            pl.BlockSpec((1, features, tile), lambda i: (0, 0, i)),
            pl.BlockSpec((1, features, tile), lambda i: (0, 0, i)),
            pl.BlockSpec((1, tile, features), lambda i: (0, i, 0)),
        ]
        + [whole] * pieces,
        out_specs=[pl.BlockSpec(piece, lambda i: (0, 0))] * (pieces * parts),
        out_shape=[jax.ShapeDtypeStruct(piece, BF16)] * (pieces * parts),
        scratch_shapes=[
            pltpu.VMEM((count, features), BF16),
            pltpu.VMEM((count, features), F32),
        ],
        compiler_params=pltpu.CompilerParams(vmem_limit_bytes=56 * 1024 * 1024),
        cost_estimate=pl.CostEstimate(
            flops=6 * count * features * hidden,
            bytes_accessed=2 * features * (3 * hidden + 2 * count),
            transcendentals=count * hidden,
        ),
    )(w_gate, w_up, w_down, *rows)
    return [outs[k * pieces : (k + 1) * pieces] for k in range(parts)]


def layer(planes, size, tokens, expert_ids, gate_scores, w_gate, w_up, w_down):
    width = size // planes
    token_count, features = tokens.shape
    top_count = expert_ids.shape[1]
    capacity = 5 * token_count * top_count // (4 * size)
    me = lax.axis_index(AXES)
    plane, place = me // width, me % width
    xor = width & (width - 1) == 0

    def partner(spot, step):
        return spot ^ step if xor else (spot + step) % width

    def along(x, step):
        return lax.ppermute(x, AXES, [(i, (i + step * width) % size) for i in range(size)])

    def across(x, step, back):
        pairs = [(i, i // width * width + partner(i % width, step)) for i in range(size)]
        return lax.ppermute(x, AXES, [p[::-1] for p in pairs] if back else pairs)

    experts = jnp.arange(size, dtype=jnp.int32)
    experts = experts // width * width + partner(place, experts % width)
    match = expert_ids.T[None, :, :] == experts[:, None, None]
    named = jnp.any(match, axis=1)
    score = jnp.sum(jnp.where(match, gate_scores.T[None, :, :], 0.0), axis=1)
    earlier = jnp.triu(jnp.ones((token_count, token_count), BF16), 1)
    rank = jnp.dot(named.astype(BF16), earlier, preferred_element_type=F32)
    rank = jnp.where(named, rank, -1.0)
    table = jnp.stack([rank.reshape(planes, width, -1), score.reshape(planes, width, -1)], axis=1)
    table = table.reshape(planes, 2 * width, token_count)

    def facts_of(target):
        return lax.dynamic_index_in_dim(table, target, 0, keepdims=False)

    blocks, facts = [tokens], [facts_of(plane)]
    for s in range(1, planes):
        facts.append(along(facts_of((plane + s) % planes), s))
    for _ in range(1, planes):
        blocks.append(along(blocks[-1], 1))

    outputs = []
    for s in range(planes):
        rows = pack(facts[s], blocks[s], capacity)
        rows = [rows[0]] + [across(rows[m], m, False) for m in range(1, width)]
        outputs.append(ffn(rows, w_gate, w_up, w_down, parts_of(s, planes)))

    def returned(s):
        return [
            [rows[0]] + [across(rows[m], m, True) for m in range(1, width)]
            for rows in outputs[s]
        ]

    step = features // HALVES
    others = [[] for _ in range(HALVES)]
    for s in range(1, planes):
        parts = returned(s)
        for half in range(HALVES):
            rows = parts[half] if len(parts) > 1 else parts[0]
            first = half if len(parts) == 1 else 0
            piece = mix(facts[s], rows, others[half], capacity, step, first, 1)
            others[half] = [along(piece, 1)]
    return mix(facts[0], returned(0)[0], sum(others, []), capacity, step, 0, HALVES)


def solution(mesh):
    split = P(AXES, None)
    whole = P(AXES, None, None)
    planes, size = planes_of(mesh), mesh.devices.size

    def step(*arrays):
        return layer(planes, size, *arrays)

    return jax.shard_map(
        step,
        mesh=mesh,
        in_specs=(split, split, split, whole, whole, whole),
        out_specs=split,
        check_vma=False,
    )
```
